32 devices in a mesh: gx: 4 (over x, core), gy: 4 (over z), gz: 2 (over y).
Axes of the slice: x: 2, y: 2, z: 4, core: 2. Of those that a mesh axis runs over, the one named last changes fastest.
Arguments:
- orbitals: float32 [64, 32, 32, 256], P(None, 'gx', 'gy', 'gz'), may hold values from -6 to 6
- potential: float32 [32, 32, 256], P('gx', 'gy', 'gz'), may hold values from 0 to 0.5
- centre: float32 [64], replicated, may hold values from 3 to 5
- half_width: float32 [64], replicated, may hold values from 3 to 5
Outputs:
- filtered: float32 [64, 32, 32, 256], P(None, 'gx', 'gy', 'gz')
The draws below stay inside these ranges and needn't reach their ends.
All inputs are finite; a program needn't handle non-finite values.
Results may differ from the reference program's by a relative error of at most 0.00002.
Values sent between devices are 32-bit elements; how exact they have to be, the bound alone decides.
A program may use at most 64 MiB of HBM per device.

```python
import jax
import jax.numpy as jnp
from jax import lax

BANDS = 64
NX = 32
NY = 32
NZ = 256


def block_levels(rng, shape, split, least, top_value):
    def one(axis_at, blocks):
        heights = jax.random.uniform(jax.random.fold_in(jax.random.fold_in(rng, 6), axis_at), (blocks,), jnp.float32, least / len(split), top_value / len(split))
        return jnp.repeat(jnp.exp(heights), shape[axis_at] // blocks).reshape((-1,) + (1,) * (len(shape) - axis_at - 1))

    level = one(*split[0])
    for cut in split[1:]:
        level = level * one(*cut)
    return level


def gaussian(stream_key, dims, scale, bound, split=(), dtype=jnp.bfloat16):
    result = jax.random.normal(stream_key, dims, jnp.float32) * scale
    if len(split) > 0:
        result = block_levels(stream_key, dims, split, -0.22, 0.18) * result
    return jnp.clip(result, min=-bound, max=bound).astype(dtype)


def setup_inputs(seed: int = 0) -> dict:
    key_of = jax.random.split(jax.random.key(seed), 5)
    orbitals = gaussian(key_of[0], (BANDS, NX, NY, NZ), 1.0, 6.0, ((1, 4), (2, 4), (3, 2)), jnp.float32)
    potential = jnp.clip(0.5 * jax.random.uniform(key_of[1], (NX, NY, NZ), jnp.float32) ** block_levels(key_of[1], (NX, NY, NZ), ((0, 4), (1, 4), (2, 2)), -0.2, 0.2), 0.0, 0.5)
    centre = jnp.clip(jax.random.uniform(key_of[2], (BANDS,), jnp.float32, 3.0, 5.0), 3.0, 5.0)
    half_width = jnp.clip(jax.random.uniform(key_of[3], (BANDS,), jnp.float32, 3.0, 5.0), 3.0, 5.0)
    return {"orbitals": orbitals, "potential": potential, "centre": centre, "half_width": half_width}


shift_mass = 0.05
jacobi_weight = 2.0 / 3.0


def neighbour_sum(field):
    total = jnp.roll(field, 1, 0) + jnp.roll(field, -1, 0)
    total = total + jnp.roll(field, 1, 1) + jnp.roll(field, -1, 1)
    return total + jnp.roll(field, 1, 2) + jnp.roll(field, -1, 2)


def operate(field, diagonal, coupling):
    return diagonal * field - coupling * neighbour_sum(field)


def restrict(field):
    shape = field.shape
    return 0.5 * field.reshape(shape[0] // 2, 2, shape[1] // 2, 2, shape[2] // 2, 2).sum(axis=(1, 3, 5))


def average_cells(field):
    shape = field.shape
    return 0.125 * field.reshape(shape[0] // 2, 2, shape[1] // 2, 2, shape[2] // 2, 2).sum(axis=(1, 3, 5))


def prolong(field):
    return jnp.repeat(jnp.repeat(jnp.repeat(field, 2, 0), 2, 1), 2, 2)


def relax(level, source, diagonal, coupling):
    return level + jacobi_weight * (source - operate(level, diagonal, coupling)) / diagonal


def reference(orbitals, potential, centre, half_width):
    potential_one = average_cells(potential)
    potential_two = average_cells(potential_one)
    diagonal_fine = 3.0 + potential
    diagonal_one = 0.75 + potential_one + shift_mass
    diagonal_two = 0.1875 + potential_two + shift_mass

    def one_band(packed):
        orbital, middle, spread = packed
        first_image = operate(orbital, diagonal_fine, 0.5)
        first_order = (first_image - middle * orbital) / spread
        second_image = operate(first_order, diagonal_fine, 0.5)
        second_order = 2.0 * (second_image - middle * first_order) / spread - orbital
        source_one = restrict(second_order)
        level_one = jacobi_weight * source_one / diagonal_one
        level_one = relax(level_one, source_one, diagonal_one, 0.125)
        residue = source_one - operate(level_one, diagonal_one, 0.125)
        source_two = restrict(residue)
        level_two = jacobi_weight * source_two / diagonal_two
        for sweep_index in range(2):
            level_two = relax(level_two, source_two, diagonal_two, 0.03125)
        level_one = level_one + prolong(level_two)
        level_one = relax(level_one, source_one, diagonal_one, 0.125)
        return second_order + prolong(level_one)

    return lax.map(one_band, (orbitals, centre, half_width))
```

```python
import functools

import jax
import jax.numpy as jnp
from jax import lax
from jax.experimental import pallas as pl
from jax.experimental.pallas import tpu as pltpu
from jax.sharding import PartitionSpec as P

shift_mass = 0.05
jacobi_weight = 2.0 / 3.0
MESH = pl.DeviceIdType.MESH
ORB, FIRST, LEV_A, LEV_B, TWO_A, TWO_B, TWO_C = range(7)


def kernel(sizes, chunks, centre, half_width, pot, orbitals, out, *scratch):
    ext = scratch[0:7]
    second, zsend, zrecv, band_a, band_i, pot_b, d1_b, r1_b, r2_b = scratch[7:16]
    load_sem, store_sem, send_sem, recv_sem = scratch[16:20]
    bands, nx, ny, nz = second.shape[2], second.shape[0], second.shape[1], second.shape[3]
    width = bands // chunks
    groups = width // 8
    two_sided = sizes["gz"] > 2
    dims = [(nx, ny, 1)] * 2 + [(nx // 2, ny // 2, 2)] * 2 + [(nx // 4, ny // 4, 4)] * 3
    lane = lax.broadcasted_iota(jnp.int32, (8, nz), 1)
    sub = lax.broadcasted_iota(jnp.int32, (8, nz), 0)

    near = {}
    for axis in ("gx", "gy", "gz"):
        me, n = lax.axis_index(axis), sizes[axis]
        near[axis] = ({axis: lax.rem(me + n - 1, n)}, {axis: lax.rem(me + 1, n)})
    peers = [near["gx"][0], near["gx"][1], near["gy"][0], near["gy"][1], near["gz"][1]]
    if two_sided:
        peers.append(near["gz"][0])

    def loads(k):
        rows = pl.ds(pl.multiple_of(k * width, 8), width)

        def line(x, _):
            for y in range(ny):
                pltpu.make_async_copy(
                    orbitals.at[rows, x, y], ext[ORB].at[x + 1, y + 1, rows], load_sem.at[k]
                ).start()
            return 0

        lax.fori_loop(0, nx, line, 0)

    lax.fori_loop(0, chunks, lambda k, c: (loads(k), c)[1], 0)

    barrier = pltpu.get_barrier_semaphore()
    for peer in peers:
        pl.semaphore_signal(barrier, inc=1, device_id=peer, device_id_type=MESH)

    def copies(p, k):
        mx, my, _ = dims[p]
        e = ext[p]
        rows = pl.ds(pl.multiple_of(k * width, 8), width)
        ys, xs = pl.ds(1, my), pl.ds(1, mx)
        moves = [
            (e.at[1, ys, rows], e.at[mx + 1, ys, rows], near["gx"][0]),
            (e.at[mx, ys, rows], e.at[0, ys, rows], near["gx"][1]),
            (e.at[xs, 1, rows], e.at[xs, my + 1, rows], near["gy"][0]),
            (e.at[xs, my, rows], e.at[xs, 0, rows], near["gy"][1]),
            (zsend.at[p, rows], zrecv.at[p, 0, rows], near["gz"][1]),
        ]
        if two_sided:
            moves.append((zsend.at[p, rows], zrecv.at[p, 1, rows], near["gz"][0]))
        return [
            pltpu.make_async_remote_copy(
                src_ref=src,
                dst_ref=dst,
                send_sem=send_sem.at[p, k, j],
                recv_sem=recv_sem.at[p, k, j],
                device_id=to,
                device_id_type=MESH,
            )
            for j, (src, dst, to) in enumerate(moves)
        ]

    def send(p, k):
        for copy in copies(p, k):
            copy.start()

    def receive(p, k):
        for copy in copies(p, k):
            copy.wait_recv()

    def roll(v, shift):
        return pltpu.roll(v, shift % nz, v.ndim - 1)

    def pack(p, get):
        mx, my, w = dims[p]
        acc = jnp.zeros((8, nz), jnp.float32)
        for x in range(mx):
            for y in range(my):
                at = 2 * w * (x * my + y)
                here = (lane >= at) & (lane < at + 2 * w)
                acc = jnp.where(here, roll(get(x, y), at + w), acc)
        return acc

    def pack_store(p, sl):
        zsend[p, sl] = pack(p, lambda x, y: ext[p][x + 1, y + 1, sl])

    def edges(p, sl):
        w = dims[p][2]
        got = zrecv[p, 0, sl]
        if two_sided:
            got = jnp.where(lax.rem(lane, 2 * w) < w, got, zrecv[p, 1, sl])
        return got

    def edge_at(p, got, x, y):
        _, my, w = dims[p]
        return roll(got, -(2 * w * (x * my + y)) - w)

    def along_z(v, h, w):
        low = roll(jnp.where(lane[None] >= nz - w, h, v), w)
        high = roll(jnp.where(lane[None] < w, h, v), -w)
        return low + high

    def around(p, sl, got, x):
        _, my, w = dims[p]
        e = ext[p]
        c = e[x + 1, pl.ds(1, my), sl]
        total = e[x, pl.ds(1, my), sl] + e[x + 2, pl.ds(1, my), sl]
        total = total + (e[x + 1, pl.ds(0, my), sl] + e[x + 1, pl.ds(2, my), sl])
        h = jnp.stack([edge_at(p, got, x, y) for y in range(my)])
        return c, total + along_z(c, h, w)

    def pair_sum(v, w):
        even = lax.rem(lane, 2 * w) < w
        return v + jnp.where(even, roll(v, -w), roll(v, w))

    def each(body, p_in, p_out):
        def one(k, carry):
            if p_in is not None:
                receive(p_in, k)
            for gg in range(groups) if groups == 1 else [None]:
                if gg is None:
                    def inner(i, c):
                        body(pl.ds(pl.multiple_of(k * width + i * 8, 8), 8))
                        return c
                    lax.fori_loop(0, groups, inner, 0)
                else:
                    body(pl.ds(pl.multiple_of(k * width, 8), 8))
            if p_out is not None:
                send(p_out, k)
            return carry

        lax.fori_loop(0, chunks, one, 0)

    for g in range(bands // 8):
        m = jnp.zeros((8, nz), jnp.float32)
        s = jnp.ones((8, nz), jnp.float32)
        for j in range(8):
            m = jnp.where(sub == j, centre[g * 8 + j], m)
            s = jnp.where(sub == j, half_width[g * 8 + j], s)
        band_a[pl.ds(g * 8, 8)] = 3.0 - m
        band_i[pl.ds(g * 8, 8)] = 1.0 / s
    for x in range(nx):
        for y in range(ny):
            pot_b[x, y] = jnp.broadcast_to(pot[x, pl.ds(y, 1), :], (8, nz))
    for qx in range(nx // 4):
        for qy in range(ny // 4):
            quad = jnp.zeros((8, nz), jnp.float32)
            for hx in range(2):
                for hy in range(2):
                    x, y = 2 * qx + hx, 2 * qy + hy
                    v = pot_b[2 * x, 2 * y] + pot_b[2 * x + 1, 2 * y]
                    v = v + (pot_b[2 * x, 2 * y + 1] + pot_b[2 * x + 1, 2 * y + 1])
                    one = 0.125 * pair_sum(v, 1)
                    quad = quad + one
                    d1 = 0.75 + one + shift_mass
                    d1_b[x, y] = d1
                    r1_b[x, y] = jacobi_weight / d1
            r2_b[qx, qy] = jacobi_weight / (0.1875 + 0.125 * pair_sum(quad, 2) + shift_mass)

    pl.semaphore_wait(barrier, len(peers))

    def start(k, carry):
        rows = pl.ds(pl.multiple_of(k * width, 8), width)
        whole = ext[ORB].at[pl.ds(1, nx), pl.ds(1, ny), rows]
        pltpu.make_async_copy(whole, whole, load_sem.at[k]).wait()

        def inner(i, c):
            pack_store(ORB, pl.ds(pl.multiple_of(k * width + i * 8, 8), 8))
            return c

        lax.fori_loop(0, groups, inner, 0)
        send(ORB, k)
        return carry

    lax.fori_loop(0, chunks, start, 0)

    def step_first(sl):
        got = edges(ORB, sl)
        a, i = band_a[sl], band_i[sl]
        for x in range(nx):
            c, total = around(ORB, sl, got, x)
            ext[FIRST][x + 1, pl.ds(1, ny), sl] = ((pot_b[x] + a) * c - 0.5 * total) * i
        pack_store(FIRST, sl)

    each(step_first, ORB, FIRST)

    def step_second(sl):
        got = edges(FIRST, sl)
        a, i = band_a[sl], 2.0 * band_i[sl]
        for x2 in range(nx // 2):
            pair = None
            for x in (2 * x2, 2 * x2 + 1):
                c, total = around(FIRST, sl, got, x)
                v = ((pot_b[x] + a) * c - 0.5 * total) * i - ext[ORB][x + 1, pl.ds(1, ny), sl]
                second[x, :, sl] = v
                pair = v if pair is None else pair + v
            for y2 in range(ny // 2):
                s = 0.5 * pair_sum(pair[2 * y2] + pair[2 * y2 + 1], 1)
                ext[LEV_A][x2 + 1, y2 + 1, sl] = r1_b[x2, y2] * s
        pack_store(LEV_A, sl)

    each(step_second, FIRST, LEV_A)

    def step_level(sl):
        got = edges(LEV_A, sl)
        for x in range(nx // 2):
            c, total = around(LEV_A, sl, got, x)
            ext[LEV_B][x + 1, pl.ds(1, ny // 2), sl] = (
                (2.0 - jacobi_weight) * c + 0.125 * r1_b[x] * total
            )
        pack_store(LEV_B, sl)

    each(step_level, LEV_A, LEV_B)

    def step_residue(sl):
        got = edges(LEV_B, sl)
        for x2 in range(nx // 4):
            pair = None
            for x in (2 * x2, 2 * x2 + 1):
                c, total = around(LEV_B, sl, got, x)
                d = d1_b[x]
                source = ext[LEV_A][x + 1, pl.ds(1, ny // 2), sl] * (d * (1.0 / jacobi_weight))
                v = source - d * c + 0.125 * total
                pair = v if pair is None else pair + v
            for y2 in range(ny // 4):
                s = 0.5 * pair_sum(pair[2 * y2] + pair[2 * y2 + 1], 2)
                ext[TWO_A][x2 + 1, y2 + 1, sl] = r2_b[x2, y2] * s
        pack_store(TWO_A, sl)

    each(step_residue, LEV_B, TWO_A)

    def step_two(sl):
        got = edges(TWO_A, sl)
        for x in range(nx // 4):
            c, total = around(TWO_A, sl, got, x)
            ext[TWO_B][x + 1, pl.ds(1, ny // 4), sl] = (
                (2.0 - jacobi_weight) * c + 0.03125 * r2_b[x] * total
            )
        pack_store(TWO_B, sl)

    each(step_two, TWO_A, TWO_B)

    def step_two_again(sl):
        got = edges(TWO_B, sl)
        for x in range(nx // 4):
            c, total = around(TWO_B, sl, got, x)
            scaled = ext[TWO_A][x + 1, pl.ds(1, ny // 4), sl]
            ext[TWO_C][x + 1, pl.ds(1, ny // 4), sl] = (
                (1.0 - jacobi_weight) * c + scaled + 0.03125 * r2_b[x] * total
            )
        pack_store(TWO_C, sl)

    each(step_two_again, TWO_B, TWO_C)

    def step_last(sl):
        hx, hy = nx // 2, ny // 2
        fine, coarse = ext[LEV_B], ext[TWO_C]

        def at(x, y):
            return fine[x + 1, y + 1, sl] + coarse[(x + 2) // 2, (y + 2) // 2, sl]

        got_one, got_two = edges(LEV_B, sl), edges(TWO_C, sl)
        for x in range(hx):
            for y in range(hy):
                c = at(x, y)
                total = (at(x - 1, y) + at(x + 1, y)) + (at(x, y - 1) + at(x, y + 1))
                h = edge_at(LEV_B, got_one, x, y) + edge_at(TWO_C, got_two, x // 2, y // 2)
                total = total + along_z(c[None], h[None], 2)[0]
                v = (1.0 - jacobi_weight) * c + ext[LEV_A][x + 1, y + 1, sl]
                v = v + 0.125 * r1_b[x, y] * total
                for i in range(2):
                    for j in range(2):
                        fx, fy = 2 * x + i, 2 * y + j
                        second[fx, fy, sl] = second[fx, fy, sl] + v

    def finish(k, carry):
        rows = pl.ds(pl.multiple_of(k * width, 8), width)
        receive(TWO_C, k)

        def inner(i, c):
            step_last(pl.ds(pl.multiple_of(k * width + i * 8, 8), 8))
            return c

        lax.fori_loop(0, groups, inner, 0)

        def line(x, c):
            for y in range(ny):
                pltpu.make_async_copy(
                    second.at[x, y, rows], out.at[rows, x, y], store_sem.at[k]
                ).start()
            return c

        lax.fori_loop(0, nx, line, 0)
        return carry

    lax.fori_loop(0, chunks, finish, 0)

    def drain(k, carry):
        rows = pl.ds(pl.multiple_of(k * width, 8), width)
        for p in range(7):
            for copy in copies(p, k):
                copy.wait_send()
        whole = second.at[:, :, rows]
        pltpu.make_async_copy(whole, whole, store_sem.at[k]).wait()
        return carry

    lax.fori_loop(0, chunks, drain, 0)


def local(sizes, chunks, orbitals, potential, centre, half_width):
    bands, nx, ny, nz = orbitals.shape

    def f32(*shape):
        return pltpu.VMEM(shape, jnp.float32)

    def padded(cut):
        return f32(nx // cut + 2, ny // cut + 2, bands, nz)

    scratch = [padded(1)] * 2 + [padded(2)] * 2 + [padded(4)] * 3
    scratch += [
        f32(nx, ny, bands, nz),
        f32(7, bands, nz),
        f32(7, 2, bands, nz),
        f32(bands, nz),
        f32(bands, nz),
        f32(nx, ny, 8, nz),
        f32(nx // 2, ny // 2, 8, nz),
        f32(nx // 2, ny // 2, 8, nz),
        f32(nx // 4, ny // 4, 8, nz),
        pltpu.SemaphoreType.DMA((chunks,)),
        pltpu.SemaphoreType.DMA((chunks,)),
        pltpu.SemaphoreType.DMA((7, chunks, 6)),
        pltpu.SemaphoreType.DMA((7, chunks, 6)),
    ]
    return pl.pallas_call(
        functools.partial(kernel, sizes, chunks),
        out_shape=jax.ShapeDtypeStruct(orbitals.shape, jnp.float32),
        in_specs=[
            pl.BlockSpec(memory_space=pltpu.SMEM),
            pl.BlockSpec(memory_space=pltpu.SMEM),
            pl.BlockSpec(memory_space=pltpu.VMEM),
            pl.BlockSpec(memory_space=pl.ANY),
        ],
        out_specs=pl.BlockSpec(memory_space=pl.ANY),
        scratch_shapes=scratch,
        compiler_params=pltpu.CompilerParams(
            collective_id=0, has_side_effects=True, vmem_limit_bytes=48 * 1024 * 1024
        ),
    )(centre, half_width, potential, orbitals)


def solution(mesh):
    in_specs = (P(None, "gx", "gy", "gz"), P("gx", "gy", "gz"), P(), P())
    out_specs = P(None, "gx", "gy", "gz")
    body = functools.partial(local, dict(mesh.shape), 4)
    return jax.shard_map(body, mesh=mesh, in_specs=in_specs, out_specs=out_specs, check_vma=False)
```

```python
import functools

import jax
import jax.numpy as jnp
from jax import lax
from jax.experimental import pallas as pl
from jax.experimental.pallas import tpu as pltpu
from jax.sharding import PartitionSpec as P

shift_mass = 0.05
jacobi_weight = 2.0 / 3.0
MESH = pl.DeviceIdType.MESH
ORB, FIRST, LEV_A, LEV_B, TWO_A, TWO_B, TWO_C = range(7)


def kernel(sizes, chunks, centre_in, half_width_in, pot_in, orbitals, out, *scratch):
    ext = scratch[0:7]
    second, zsend, zrecv, band_a, band_i, pot_b, d1_b, r1_b, r2_b = scratch[7:16]
    load_sem, store_sem, send_sem, recv_sem = scratch[16:20]
    centre, half_width, pot, small_sem = scratch[20:24]
    packed_out, packed_in = scratch[24:29], scratch[29:34]
    bands, nx, ny, nz = second.shape[2], second.shape[0], second.shape[1], second.shape[3]
    width = bands // chunks
    groups = width // 8
    two_sided = sizes["gz"] > 2
    dims = [(nx, ny, 1)] * 2 + [(nx // 2, ny // 2, 2)] * 2 + [(nx // 4, ny // 4, 4)] * 3
    lane = lax.broadcasted_iota(jnp.int32, (8, nz), 1)
    sub = lax.broadcasted_iota(jnp.int32, (8, nz), 0)

    near = {}
    for axis in ("gx", "gy", "gz"):
        me, n = lax.axis_index(axis), sizes[axis]
        near[axis] = ({axis: lax.rem(me + n - 1, n)}, {axis: lax.rem(me + 1, n)})
    peers = [near["gx"][0], near["gx"][1], near["gy"][0], near["gy"][1], near["gz"][1]]
    if two_sided:
        peers.append(near["gz"][0])

    smalls = [
        pltpu.make_async_copy(src, dst, small_sem.at[j])
        for j, (src, dst) in enumerate(
            [(centre_in, centre), (half_width_in, half_width), (pot_in, pot)]
        )
    ]

    def loads(k):
        rows = pl.ds(pl.multiple_of(k * width, 8), width)

        def line(x, _):
            for y in range(ny):
                pltpu.make_async_copy(
                    orbitals.at[rows, x, y], ext[ORB].at[x + 1, y + 1, rows], load_sem.at[k]
                ).start()
            return 0

        lax.fori_loop(0, nx, line, 0)

    lax.fori_loop(0, chunks, lambda k, c: (loads(k), c)[1], 0)
    for small in smalls:
        small.start()

    barrier = pltpu.get_barrier_semaphore()
    for peer in peers:
        pl.semaphore_signal(barrier, inc=1, device_id=peer, device_id_type=MESH)

    def copies(p, k):
        mx, my, _ = dims[p]
        e = ext[p]
        rows = pl.ds(pl.multiple_of(k * width, 8), width)
        ys, xs = pl.ds(1, my), pl.ds(1, mx)
        if p in (ORB, FIRST):
            moves = [
                (e.at[xs, 1, rows], e.at[xs, my + 1, rows], near["gy"][0]),
                (e.at[xs, my, rows], e.at[xs, 0, rows], near["gy"][1]),
                (e.at[1, ys, rows], e.at[mx + 1, ys, rows], near["gx"][0]),
                (e.at[mx, ys, rows], e.at[0, ys, rows], near["gx"][1]),
            ]
        else:
            share = width if p in (LEV_A, LEV_B) else width // 2
            part = pl.ds(pl.multiple_of(k * share, 8), share)
            sent, got = packed_out[p - LEV_A], packed_in[p - LEV_A]
            moves = [
                (sent.at[j, :, part], got.at[j, :, part], near[axis][side])
                for j, (axis, side) in enumerate(
                    [("gy", 0), ("gy", 1), ("gx", 0), ("gx", 1)]
                )
            ]
        moves.append((zsend.at[p, rows], zrecv.at[p, 0, rows], near["gz"][1]))
        if two_sided:
            moves.append((zsend.at[p, rows], zrecv.at[p, 1, rows], near["gz"][0]))
        return [
            pltpu.make_async_remote_copy(
                src_ref=src,
                dst_ref=dst,
                send_sem=send_sem.at[p, k, j],
                recv_sem=recv_sem.at[p, k, j],
                device_id=to,
                device_id_type=MESH,
            )
            for j, (src, dst, to) in enumerate(moves)
        ]

    def items(p, k):
        mx, my, w = dims[p]
        base = k * width
        if w == 2:
            for i in range(width // 8):
                at = pl.ds(pl.multiple_of(base + 8 * i, 8), 8)
                for pair in range(mx // 2):
                    yield pair, at, [(2 * pair, at), (2 * pair + 1, at)]
        else:
            for i in range(width // 16):
                rows = [pl.ds(pl.multiple_of(base + 16 * i + 8 * h, 8), 8) for h in (0, 1)]
                at = pl.ds(pl.multiple_of(k * (width // 2) + 8 * i, 8), 8)
                for pair in range(mx // 2):
                    yield pair, at, [(2 * pair + c, r) for r in rows for c in (0, 1)]

    def face_cell(p, j, cell, halo):
        mx, my, _ = dims[p]
        if j < 2:
            return (cell + 1, ((my + 1, 0) if halo else (1, my))[j])
        return (((mx + 1, 0) if halo else (1, mx))[j - 2], cell + 1)

    def send(p, k):
        if p not in (ORB, FIRST):
            w = dims[p][2]
            for pair, at, parts in items(p, k):
                for j in range(4):
                    acc = None
                    for spot, (cell, r) in enumerate(parts):
                        cx, cy = face_cell(p, j, cell, False)
                        v = ext[p][cx, cy, r]
                        acc = v if acc is None else jnp.where(lax.rem(lane, w) == spot, v, acc)
                    packed_out[p - LEV_A][j, pair, at] = acc
        for copy in copies(p, k):
            copy.start()

    def receive(p, k):
        for copy in copies(p, k):
            copy.wait_recv()
        if p not in (ORB, FIRST):
            w = dims[p][2]
            for pair, at, parts in items(p, k):
                for j in range(4):
                    got = packed_in[p - LEV_A][j, pair, at]
                    for spot, (cell, r) in enumerate(parts):
                        cx, cy = face_cell(p, j, cell, True)
                        v = jnp.where(lax.rem(lane, w) == spot, got, 0.0)
                        reach = 1
                        while reach < w:
                            v = v + roll(v, -reach if spot & reach else reach)
                            reach *= 2
                        ext[p][cx, cy, r] = v

    def roll(v, shift):
        return pltpu.roll(v, shift % nz, v.ndim - 1)

    def pack(p, get):
        mx, my, w = dims[p]
        acc = jnp.zeros((8, nz), jnp.float32)
        for x in range(mx):
            for y in range(my):
                at = 2 * w * (x * my + y)
                here = (lane >= at) & (lane < at + 2 * w)
                acc = jnp.where(here, roll(get(x, y), at + w), acc)
        return acc

    def pack_store(p, sl):
        zsend[p, sl] = pack(p, lambda x, y: ext[p][x + 1, y + 1, sl])

    def edges(p, sl):
        w = dims[p][2]
        got = zrecv[p, 0, sl]
        if two_sided:
            got = jnp.where(lax.rem(lane, 2 * w) < w, got, zrecv[p, 1, sl])
        return got

    def edge_at(p, got, x, y):
        _, my, w = dims[p]
        return roll(got, -(2 * w * (x * my + y)) - w)

    def along_z(v, h, w):
        low = roll(jnp.where(lane[None] >= nz - w, h, v), w)
        high = roll(jnp.where(lane[None] < w, h, v), -w)
        return low + high

    def around(p, sl, got, x):
        _, my, w = dims[p]
        e = ext[p]
        c = e[x + 1, pl.ds(1, my), sl]
        total = e[x, pl.ds(1, my), sl] + e[x + 2, pl.ds(1, my), sl]
        total = total + (e[x + 1, pl.ds(0, my), sl] + e[x + 1, pl.ds(2, my), sl])
        h = jnp.stack([edge_at(p, got, x, y) for y in range(my)])
        return c, total + along_z(c, h, w)

    def pair_sum(v, w):
        even = lax.rem(lane, 2 * w) < w
        return v + jnp.where(even, roll(v, -w), roll(v, w))

    def each(body, p_in, p_out):
        def one(k, carry):
            if p_in is not None:
                receive(p_in, k)

            def inner(i, c):
                body(pl.ds(pl.multiple_of(k * width + i * 8, 8), 8))
                return c

            lax.fori_loop(0, groups, inner, 0)
            if p_out is not None:
                send(p_out, k)
            return carry

        lax.fori_loop(0, chunks, one, 0)

    pl.semaphore_wait(barrier, len(peers))

    def start(k, carry):
        rows = pl.ds(pl.multiple_of(k * width, 8), width)
        whole = ext[ORB].at[pl.ds(1, nx), pl.ds(1, ny), rows]
        pltpu.make_async_copy(whole, whole, load_sem.at[k]).wait()

        moves = copies(ORB, k)
        for copy in moves[:4]:
            copy.start()

        def inner(i, c):
            pack_store(ORB, pl.ds(pl.multiple_of(k * width + i * 8, 8), 8))
            return c

        lax.fori_loop(0, groups, inner, 0)
        for copy in moves[4:]:
            copy.start()
        return carry

    lax.fori_loop(0, chunks, start, 0)

    for small in smalls:
        small.wait()
    for g in range(bands // 8):
        m = jnp.zeros((8, nz), jnp.float32)
        s = jnp.ones((8, nz), jnp.float32)
        for j in range(8):
            m = jnp.where(sub == j, centre[g * 8 + j], m)
            s = jnp.where(sub == j, half_width[g * 8 + j], s)
        band_a[pl.ds(g * 8, 8)] = 3.0 - m
        band_i[pl.ds(g * 8, 8)] = 1.0 / s
    for x in range(nx):
        for y in range(ny):
            pot_b[x, y] = jnp.broadcast_to(pot[x, pl.ds(y, 1), :], (8, nz))
    for qx in range(nx // 4):
        for qy in range(ny // 4):
            quad = jnp.zeros((8, nz), jnp.float32)
            for hx in range(2):
                for hy in range(2):
                    x, y = 2 * qx + hx, 2 * qy + hy
                    v = pot_b[2 * x, 2 * y] + pot_b[2 * x + 1, 2 * y]
                    v = v + (pot_b[2 * x, 2 * y + 1] + pot_b[2 * x + 1, 2 * y + 1])
                    one = 0.125 * pair_sum(v, 1)
                    quad = quad + one
                    d1 = 0.75 + one + shift_mass
                    d1_b[x, y] = d1
                    r1_b[x, y] = jacobi_weight / d1
            r2_b[qx, qy] = jacobi_weight / (0.1875 + 0.125 * pair_sum(quad, 2) + shift_mass)

    def step_first(sl):
        got = edges(ORB, sl)
        a, i = band_a[sl], band_i[sl]
        for x in range(nx):
            c, total = around(ORB, sl, got, x)
            ext[FIRST][x + 1, pl.ds(1, ny), sl] = ((pot_b[x] + a) * c - 0.5 * total) * i
        pack_store(FIRST, sl)

    each(step_first, ORB, FIRST)

    def step_second(sl):
        got = edges(FIRST, sl)
        a, i = band_a[sl], 2.0 * band_i[sl]
        for x2 in range(nx // 2):
            pair = None
            for x in (2 * x2, 2 * x2 + 1):
                c, total = around(FIRST, sl, got, x)
                v = ((pot_b[x] + a) * c - 0.5 * total) * i - ext[ORB][x + 1, pl.ds(1, ny), sl]
                second[x, :, sl] = v
                pair = v if pair is None else pair + v
            for y2 in range(ny // 2):
                s = 0.5 * pair_sum(pair[2 * y2] + pair[2 * y2 + 1], 1)
                ext[LEV_A][x2 + 1, y2 + 1, sl] = r1_b[x2, y2] * s
        pack_store(LEV_A, sl)

    each(step_second, FIRST, LEV_A)

    def step_level(sl):
        got = edges(LEV_A, sl)
        for x in range(nx // 2):
            c, total = around(LEV_A, sl, got, x)
            ext[LEV_B][x + 1, pl.ds(1, ny // 2), sl] = (
                (2.0 - jacobi_weight) * c + 0.125 * r1_b[x] * total
            )
        pack_store(LEV_B, sl)

    each(step_level, LEV_A, LEV_B)

    def step_residue(sl):
        got = edges(LEV_B, sl)
        for x2 in range(nx // 4):
            pair = None
            for x in (2 * x2, 2 * x2 + 1):
                c, total = around(LEV_B, sl, got, x)
                d = d1_b[x]
                source = ext[LEV_A][x + 1, pl.ds(1, ny // 2), sl] * (d * (1.0 / jacobi_weight))
                v = source - d * c + 0.125 * total
                pair = v if pair is None else pair + v
            for y2 in range(ny // 4):
                s = 0.5 * pair_sum(pair[2 * y2] + pair[2 * y2 + 1], 2)
                ext[TWO_A][x2 + 1, y2 + 1, sl] = r2_b[x2, y2] * s
        pack_store(TWO_A, sl)

    each(step_residue, LEV_B, TWO_A)

    def step_two(sl):
        got = edges(TWO_A, sl)
        for x in range(nx // 4):
            c, total = around(TWO_A, sl, got, x)
            ext[TWO_B][x + 1, pl.ds(1, ny // 4), sl] = (
                (2.0 - jacobi_weight) * c + 0.03125 * r2_b[x] * total
            )
        pack_store(TWO_B, sl)

    each(step_two, TWO_A, TWO_B)

    def step_two_again(sl):
        got = edges(TWO_B, sl)
        for x in range(nx // 4):
            c, total = around(TWO_B, sl, got, x)
            scaled = ext[TWO_A][x + 1, pl.ds(1, ny // 4), sl]
            ext[TWO_C][x + 1, pl.ds(1, ny // 4), sl] = (
                (1.0 - jacobi_weight) * c + scaled + 0.03125 * r2_b[x] * total
            )
        pack_store(TWO_C, sl)

    each(step_two_again, TWO_B, TWO_C)

    def step_last(sl):
        hx, hy = nx // 2, ny // 2
        fine, coarse = ext[LEV_B], ext[TWO_C]

        def at(x, y):
            return fine[x + 1, y + 1, sl] + coarse[(x + 2) // 2, (y + 2) // 2, sl]

        got_one, got_two = edges(LEV_B, sl), edges(TWO_C, sl)
        for x in range(hx):
            for y in range(hy):
                c = at(x, y)
                total = (at(x - 1, y) + at(x + 1, y)) + (at(x, y - 1) + at(x, y + 1))
                h = edge_at(LEV_B, got_one, x, y) + edge_at(TWO_C, got_two, x // 2, y // 2)
                total = total + along_z(c[None], h[None], 2)[0]
                v = (1.0 - jacobi_weight) * c + ext[LEV_A][x + 1, y + 1, sl]
                v = v + 0.125 * r1_b[x, y] * total
                for i in range(2):
                    for j in range(2):
                        fx, fy = 2 * x + i, 2 * y + j
                        second[fx, fy, sl] = second[fx, fy, sl] + v

    def finish(k, carry):
        rows = pl.ds(pl.multiple_of(k * width, 8), width)
        receive(TWO_C, k)

        def inner(i, c):
            step_last(pl.ds(pl.multiple_of(k * width + i * 8, 8), 8))
            return c

        lax.fori_loop(0, groups, inner, 0)

        def line(x, c):
            for y in range(ny):
                pltpu.make_async_copy(
                    second.at[x, y, rows], out.at[rows, x, y], store_sem.at[k]
                ).start()
            return c

        lax.fori_loop(0, nx, line, 0)
        return carry

    lax.fori_loop(0, chunks, finish, 0)

    def drain(k, carry):
        rows = pl.ds(pl.multiple_of(k * width, 8), width)
        for p in range(7):
            for copy in copies(p, k):
                copy.wait_send()
        whole = second.at[:, :, rows]
        pltpu.make_async_copy(whole, whole, store_sem.at[k]).wait()
        return carry

    lax.fori_loop(0, chunks, drain, 0)


def local(sizes, chunks, orbitals, potential, centre, half_width):
    bands, nx, ny, nz = orbitals.shape

    def f32(*shape):
        return pltpu.VMEM(shape, jnp.float32)

    def padded(cut):
        return f32(nx // cut + 2, ny // cut + 2, bands, nz)

    scratch = [padded(1)] * 2 + [padded(2)] * 2 + [padded(4)] * 3
    scratch += [
        f32(nx, ny, bands, nz),
        f32(7, bands, nz),
        f32(7, 2, bands, nz),
        f32(bands, nz),
        f32(bands, nz),
        f32(nx, ny, 8, nz),
        f32(nx // 2, ny // 2, 8, nz),
        f32(nx // 2, ny // 2, 8, nz),
        f32(nx // 4, ny // 4, 8, nz),
        pltpu.SemaphoreType.DMA((chunks,)),
        pltpu.SemaphoreType.DMA((chunks,)),
        pltpu.SemaphoreType.DMA((7, chunks, 6)),
        pltpu.SemaphoreType.DMA((7, chunks, 6)),
        pltpu.SMEM((bands,), jnp.float32),
        pltpu.SMEM((bands,), jnp.float32),
        f32(nx, ny, nz),
        pltpu.SemaphoreType.DMA((3,)),
    ]
    for _ in range(2):
        scratch += [f32(4, max(nx, ny) // 4, bands, nz)] * 2
        scratch += [f32(4, max(nx, ny) // 8, bands // 2, nz)] * 3
    return pl.pallas_call(
        functools.partial(kernel, sizes, chunks),
        out_shape=jax.ShapeDtypeStruct(orbitals.shape, jnp.float32),
        in_specs=[pl.BlockSpec(memory_space=pltpu.HBM)] * 4,
        out_specs=pl.BlockSpec(memory_space=pl.ANY),
        scratch_shapes=scratch,
        compiler_params=pltpu.CompilerParams(
            collective_id=0, has_side_effects=True, vmem_limit_bytes=67_043_328
        ),
    )(centre, half_width, potential, orbitals)


def solution(mesh):
    in_specs = (P(None, "gx", "gy", "gz"), P("gx", "gy", "gz"), P(), P())
    out_specs = P(None, "gx", "gy", "gz")
    body = functools.partial(local, dict(mesh.shape), 4)
    return jax.shard_map(body, mesh=mesh, in_specs=in_specs, out_specs=out_specs, check_vma=False)
```

```python
import functools

import jax
import jax.numpy as jnp
from jax import lax
from jax.experimental import pallas as pl
from jax.experimental.pallas import tpu as pltpu
from jax.sharding import PartitionSpec as P

shift_mass = 0.05
jacobi_weight = 2.0 / 3.0
MESH = pl.DeviceIdType.MESH
ORB, FIRST, LEV_A, LEV_B, TWO_A, TWO_B, TWO_C = range(7)


def kernel(sizes, chunks, centre_in, half_width_in, pot_in, orbitals, out, *scratch):
    ext = scratch[0:7]
    second, zsend, zrecv, band_a, band_i, pot_b, d1_b, r1_b, r2_b = scratch[7:16]
    load_sem, store_sem, send_sem, recv_sem = scratch[16:20]
    centre, half_width, pot, small_sem = scratch[20:24]
    packed_out, packed_in = scratch[24:29], scratch[29:34]
    bands, nx, ny, nz = second.shape[2], second.shape[0], second.shape[1], second.shape[3]
    width = bands // chunks
    groups = width // 8
    two_sided = sizes["gz"] > 2
    dims = [(nx, ny, 1)] * 2 + [(nx // 2, ny // 2, 2)] * 2 + [(nx // 4, ny // 4, 4)] * 3
    lane = lax.broadcasted_iota(jnp.int32, (8, nz), 1)
    sub = lax.broadcasted_iota(jnp.int32, (8, nz), 0)

    near = {}
    for axis in ("gx", "gy", "gz"):
        me, n = lax.axis_index(axis), sizes[axis]
        near[axis] = ({axis: lax.rem(me + n - 1, n)}, {axis: lax.rem(me + 1, n)})
    peers = [near["gx"][0], near["gx"][1], near["gy"][0], near["gy"][1], near["gz"][1]]
    if two_sided:
        peers.append(near["gz"][0])

    smalls = [
        pltpu.make_async_copy(src, dst, small_sem.at[j])
        for j, (src, dst) in enumerate(
            [(centre_in, centre), (half_width_in, half_width), (pot_in, pot)]
        )
    ]

    def loads(k):
        rows = pl.ds(pl.multiple_of(k * width, 8), width)

        def line(x, _):
            for y in range(ny):
                pltpu.make_async_copy(
                    orbitals.at[rows, x, y], ext[ORB].at[x + 1, y + 1, rows], load_sem.at[k]
                ).start()
            return 0

        lax.fori_loop(0, nx, line, 0)

    lax.fori_loop(0, chunks, lambda k, c: (loads(k), c)[1], 0)
    for small in smalls:
        small.start()

    barrier = pltpu.get_barrier_semaphore()
    for peer in peers:
        pl.semaphore_signal(barrier, inc=1, device_id=peer, device_id_type=MESH)

    def copies(p, k):
        mx, my, _ = dims[p]
        e = ext[p]
        rows = pl.ds(pl.multiple_of(k * width, 8), width)
        ys, xs = pl.ds(1, my), pl.ds(1, mx)
        if p in (ORB, FIRST):
            moves = [
                (e.at[xs, 1, rows], e.at[xs, my + 1, rows], near["gy"][0]),
                (e.at[xs, my, rows], e.at[xs, 0, rows], near["gy"][1]),
                (e.at[1, ys, rows], e.at[mx + 1, ys, rows], near["gx"][0]),
                (e.at[mx, ys, rows], e.at[0, ys, rows], near["gx"][1]),
            ]
        else:
            share = width if p in (LEV_A, LEV_B) else width // 2
            part = pl.ds(pl.multiple_of(k * share, 8), share)
            sent, got = packed_out[p - LEV_A], packed_in[p - LEV_A]
            moves = [
                (sent.at[j, :, part], got.at[j, :, part], near[axis][side])
                for j, (axis, side) in enumerate(
                    [("gy", 0), ("gy", 1), ("gx", 0), ("gx", 1)]
                )
            ]
        moves.append((zsend.at[p, rows], zrecv.at[p, 0, rows], near["gz"][1]))
        if two_sided:
            moves.append((zsend.at[p, rows], zrecv.at[p, 1, rows], near["gz"][0]))
        return [
            pltpu.make_async_remote_copy(
                src_ref=src,
                dst_ref=dst,
                send_sem=send_sem.at[p, k, j],
                recv_sem=recv_sem.at[p, k, j],
                device_id=to,
                device_id_type=MESH,
            )
            for j, (src, dst, to) in enumerate(moves)
        ]

    def items(p, k):
        mx, my, w = dims[p]
        base = k * width
        if w == 2:
            for i in range(width // 8):
                at = pl.ds(pl.multiple_of(base + 8 * i, 8), 8)
                for pair in range(mx // 2):
                    yield pair, at, [(2 * pair, at), (2 * pair + 1, at)]
        else:
            for i in range(width // 16):
                rows = [pl.ds(pl.multiple_of(base + 16 * i + 8 * h, 8), 8) for h in (0, 1)]
                at = pl.ds(pl.multiple_of(k * (width // 2) + 8 * i, 8), 8)
                for pair in range(mx // 2):
                    yield pair, at, [(2 * pair + c, r) for r in rows for c in (0, 1)]

    def face_cell(p, j, cell, halo):
        mx, my, _ = dims[p]
        if j < 2:
            return (cell + 1, ((my + 1, 0) if halo else (1, my))[j])
        return (((mx + 1, 0) if halo else (1, mx))[j - 2], cell + 1)

    def send(p, k):
        if p not in (ORB, FIRST):
            w = dims[p][2]
            for pair, at, parts in items(p, k):
                for j in range(4):
                    acc = None
                    for spot, (cell, r) in enumerate(parts):
                        cx, cy = face_cell(p, j, cell, False)
                        v = ext[p][cx, cy, r]
                        acc = v if acc is None else jnp.where(lax.rem(lane, w) == spot, v, acc)
                    packed_out[p - LEV_A][j, pair, at] = acc
        for copy in copies(p, k):
            copy.start()

    def receive(p, k):
        for copy in copies(p, k):
            copy.wait_recv()
        if p not in (ORB, FIRST):
            w = dims[p][2]
            for pair, at, parts in items(p, k):
                for j in range(4):
                    got = packed_in[p - LEV_A][j, pair, at]
                    for spot, (cell, r) in enumerate(parts):
                        cx, cy = face_cell(p, j, cell, True)
                        v = jnp.where(lax.rem(lane, w) == spot, got, 0.0)
                        reach = 1
                        while reach < w:
                            v = v + roll(v, -reach if spot & reach else reach)
                            reach *= 2
                        ext[p][cx, cy, r] = v

    def roll(v, shift):
        return pltpu.roll(v, shift % nz, v.ndim - 1)

    def pack(p, get):
        mx, my, w = dims[p]
        acc = jnp.zeros((8, nz), jnp.float32)
        for x in range(mx):
            for y in range(my):
                at = 2 * w * (x * my + y)
                here = (lane >= at) & (lane < at + 2 * w)
                acc = jnp.where(here, roll(get(x, y), at + w), acc)
        return acc

    def pack_store(p, sl):
        zsend[p, sl] = pack(p, lambda x, y: ext[p][x + 1, y + 1, sl])

    def edges(p, sl):
        w = dims[p][2]
        got = zrecv[p, 0, sl]
        if two_sided:
            got = jnp.where(lax.rem(lane, 2 * w) < w, got, zrecv[p, 1, sl])
        return got

    def edge_at(p, got, x, y):
        _, my, w = dims[p]
        return roll(got, -(2 * w * (x * my + y)) - w)

    def along_z(v, h, w):
        low = roll(jnp.where(lane[None] >= nz - w, h, v), w)
        high = roll(jnp.where(lane[None] < w, h, v), -w)
        return low + high

    def around(p, sl, got, x):
        _, my, w = dims[p]
        e = ext[p]
        c = e[x + 1, pl.ds(1, my), sl]
        total = e[x, pl.ds(1, my), sl] + e[x + 2, pl.ds(1, my), sl]
        total = total + (e[x + 1, pl.ds(0, my), sl] + e[x + 1, pl.ds(2, my), sl])
        h = jnp.stack([edge_at(p, got, x, y) for y in range(my)])
        return c, total + along_z(c, h, w)

    def pair_sum(v, w):
        even = lax.rem(lane, 2 * w) < w
        return v + jnp.where(even, roll(v, -w), roll(v, w))

    def each(body, p_in, p_out):
        def one(k, carry):
            if p_in is not None:
                receive(p_in, k)

            def inner(i, c):
                body(pl.ds(pl.multiple_of(k * width + i * 8, 8), 8))
                return c

            lax.fori_loop(0, groups, inner, 0)
            if p_out is not None:
                send(p_out, k)
            return carry

        lax.fori_loop(0, chunks, one, 0)

    pl.semaphore_wait(barrier, len(peers))

    def start(k, carry):
        rows = pl.ds(pl.multiple_of(k * width, 8), width)
        whole = ext[ORB].at[pl.ds(1, nx), pl.ds(1, ny), rows]
        pltpu.make_async_copy(whole, whole, load_sem.at[k]).wait()

        moves = copies(ORB, k)
        for copy in moves[:4]:
            copy.start()

        def inner(i, c):
            pack_store(ORB, pl.ds(pl.multiple_of(k * width + i * 8, 8), 8))
            return c

        lax.fori_loop(0, groups, inner, 0)
        for copy in moves[4:]:
            copy.start()
        return carry

    lax.fori_loop(0, chunks, start, 0)

    for small in smalls:
        small.wait()
    for g in range(bands // 8):
        m = jnp.zeros((8, nz), jnp.float32)
        s = jnp.ones((8, nz), jnp.float32)
        for j in range(8):
            m = jnp.where(sub == j, centre[g * 8 + j], m)
            s = jnp.where(sub == j, half_width[g * 8 + j], s)
        band_a[pl.ds(g * 8, 8)] = 3.0 - m
        band_i[pl.ds(g * 8, 8)] = 1.0 / s
    for x in range(nx):
        for y in range(ny):
            pot_b[x, y] = jnp.broadcast_to(pot[x, pl.ds(y, 1), :], (8, nz))
    for qx in range(nx // 4):
        for qy in range(ny // 4):
            quad = jnp.zeros((8, nz), jnp.float32)
            for hx in range(2):
                for hy in range(2):
                    x, y = 2 * qx + hx, 2 * qy + hy
                    v = pot_b[2 * x, 2 * y] + pot_b[2 * x + 1, 2 * y]
                    v = v + (pot_b[2 * x, 2 * y + 1] + pot_b[2 * x + 1, 2 * y + 1])
                    one = 0.125 * pair_sum(v, 1)
                    quad = quad + one
                    d1 = 0.75 + one + shift_mass
                    d1_b[x, y] = d1
                    r1_b[x, y] = jacobi_weight / d1
            r2_b[qx, qy] = jacobi_weight / (0.1875 + 0.125 * pair_sum(quad, 2) + shift_mass)

    def step_first(sl):
        got = edges(ORB, sl)
        a, i = band_a[sl], band_i[sl]
        for x in range(nx):
            c, total = around(ORB, sl, got, x)
            ext[FIRST][x + 1, pl.ds(1, ny), sl] = ((pot_b[x] + a) * c - 0.5 * total) * i
        pack_store(FIRST, sl)

    each(step_first, ORB, FIRST)

    def step_second(sl):
        got = edges(FIRST, sl)
        a, i = band_a[sl], 2.0 * band_i[sl]
        for x2 in range(nx // 2):
            pair = None
            for x in (2 * x2, 2 * x2 + 1):
                c, total = around(FIRST, sl, got, x)
                v = ((pot_b[x] + a) * c - 0.5 * total) * i - ext[ORB][x + 1, pl.ds(1, ny), sl]
                second[x, :, sl] = v
                pair = v if pair is None else pair + v
            for y2 in range(ny // 2):
                s = 0.5 * pair_sum(pair[2 * y2] + pair[2 * y2 + 1], 1)
                ext[LEV_A][x2 + 1, y2 + 1, sl] = r1_b[x2, y2] * s
        pack_store(LEV_A, sl)

    each(step_second, FIRST, LEV_A)

    def step_level(sl):
        got = edges(LEV_A, sl)
        for x in range(nx // 2):
            c, total = around(LEV_A, sl, got, x)
            ext[LEV_B][x + 1, pl.ds(1, ny // 2), sl] = (
                (2.0 - jacobi_weight) * c + 0.125 * r1_b[x] * total
            )
        pack_store(LEV_B, sl)

    each(step_level, LEV_A, LEV_B)

    def step_residue(sl):
        got = edges(LEV_B, sl)
        for x2 in range(nx // 4):
            pair = None
            for x in (2 * x2, 2 * x2 + 1):
                c, total = around(LEV_B, sl, got, x)
                d = d1_b[x]
                source = ext[LEV_A][x + 1, pl.ds(1, ny // 2), sl] * (d * (1.0 / jacobi_weight))
                v = source - d * c + 0.125 * total
                pair = v if pair is None else pair + v
            for y2 in range(ny // 4):
                s = 0.5 * pair_sum(pair[2 * y2] + pair[2 * y2 + 1], 2)
                ext[TWO_A][x2 + 1, y2 + 1, sl] = r2_b[x2, y2] * s
        pack_store(TWO_A, sl)

    each(step_residue, LEV_B, TWO_A)

    def step_two(sl):
        got = edges(TWO_A, sl)
        for x in range(nx // 4):
            c, total = around(TWO_A, sl, got, x)
            ext[TWO_B][x + 1, pl.ds(1, ny // 4), sl] = (
                (2.0 - jacobi_weight) * c + 0.03125 * r2_b[x] * total
            )
        pack_store(TWO_B, sl)

    each(step_two, TWO_A, TWO_B)

    def step_two_again(sl):
        got = edges(TWO_B, sl)
        for x in range(nx // 4):
            c, total = around(TWO_B, sl, got, x)
            scaled = ext[TWO_A][x + 1, pl.ds(1, ny // 4), sl]
            ext[TWO_C][x + 1, pl.ds(1, ny // 4), sl] = (
                (1.0 - jacobi_weight) * c + scaled + 0.03125 * r2_b[x] * total
            )
        pack_store(TWO_C, sl)

    each(step_two_again, TWO_B, TWO_C)

    def step_last(sl):
        hx, hy = nx // 2, ny // 2
        fine, coarse = ext[LEV_B], ext[TWO_C]

        def at(x, y):
            return fine[x + 1, y + 1, sl] + coarse[(x + 2) // 2, (y + 2) // 2, sl]

        got_one, got_two = edges(LEV_B, sl), edges(TWO_C, sl)
        for x in range(hx):
            for y in range(hy):
                c = at(x, y)
                total = (at(x - 1, y) + at(x + 1, y)) + (at(x, y - 1) + at(x, y + 1))
                h = edge_at(LEV_B, got_one, x, y) + edge_at(TWO_C, got_two, x // 2, y // 2)
                total = total + along_z(c[None], h[None], 2)[0]
                v = (1.0 - jacobi_weight) * c + ext[LEV_A][x + 1, y + 1, sl]
                v = v + 0.125 * r1_b[x, y] * total
                for i in range(2):
                    for j in range(2):
                        fx, fy = 2 * x + i, 2 * y + j
                        second[fx, fy, sl] = second[fx, fy, sl] + v

    def finish(k, carry):
        rows = pl.ds(pl.multiple_of(k * width, 8), width)
        receive(TWO_C, k)

        def inner(i, c):
            step_last(pl.ds(pl.multiple_of(k * width + i * 8, 8), 8))
            return c

        lax.fori_loop(0, groups, inner, 0)

        def line(x, c):
            for y in range(ny):
                pltpu.make_async_copy(
                    second.at[x, y, rows], out.at[rows, x, y], store_sem.at[k]
                ).start()
            return c

        lax.fori_loop(0, nx, line, 0)
        return carry

    lax.fori_loop(0, chunks, finish, 0)

    def drain(k, carry):
        rows = pl.ds(pl.multiple_of(k * width, 8), width)
        for p in range(7):
            for copy in copies(p, k):
                copy.wait_send()
        whole = second.at[:, :, rows]
        pltpu.make_async_copy(whole, whole, store_sem.at[k]).wait()
        return carry

    lax.fori_loop(0, chunks, drain, 0)


def local(sizes, chunks, orbitals, potential, centre, half_width):
    bands, nx, ny, nz = orbitals.shape

    def f32(*shape):
        return pltpu.VMEM(shape, jnp.float32)

    def padded(cut):
        return f32(nx // cut + 2, ny // cut + 2, bands, nz)

    scratch = [padded(1)] * 2 + [padded(2)] * 2 + [padded(4)] * 3
    scratch += [
        f32(nx, ny, bands, nz),
        f32(7, bands, nz),
        f32(7, 2, bands, nz),
        f32(bands, nz),
        f32(bands, nz),
        f32(nx, ny, 8, nz),
        f32(nx // 2, ny // 2, 8, nz),
        f32(nx // 2, ny // 2, 8, nz),
        f32(nx // 4, ny // 4, 8, nz),
        pltpu.SemaphoreType.DMA((chunks,)),
        pltpu.SemaphoreType.DMA((chunks,)),
        pltpu.SemaphoreType.DMA((7, chunks, 6)),
        pltpu.SemaphoreType.DMA((7, chunks, 6)),
        pltpu.SMEM((bands,), jnp.float32),
        pltpu.SMEM((bands,), jnp.float32),
        f32(nx, ny, nz),
        pltpu.SemaphoreType.DMA((3,)),
    ]
    for _ in range(2):
        scratch += [f32(4, max(nx, ny) // 4, bands, nz)] * 2
        scratch += [f32(4, max(nx, ny) // 8, bands // 2, nz)] * 3
    return pl.pallas_call(
        functools.partial(kernel, sizes, chunks),
        out_shape=jax.ShapeDtypeStruct(orbitals.shape, jnp.float32),
        in_specs=[pl.BlockSpec(memory_space=pltpu.HBM)] * 4,
        out_specs=pl.BlockSpec(memory_space=pl.ANY),
        scratch_shapes=scratch,
        compiler_params=pltpu.CompilerParams(
            collective_id=0, has_side_effects=True, vmem_limit_bytes=48 * 1024 * 1024
        ),
    )(*(pltpu.with_memory_space_constraint(v, pltpu.HBM) for v in (centre, half_width, potential, orbitals)))


def solution(mesh):
    in_specs = (P(None, "gx", "gy", "gz"), P("gx", "gy", "gz"), P(), P())
    out_specs = P(None, "gx", "gy", "gz")
    body = functools.partial(local, dict(mesh.shape), 4)
    return jax.shard_map(body, mesh=mesh, in_specs=in_specs, out_specs=out_specs, check_vma=False)
```

```python
import functools

import jax
import jax.numpy as jnp
from jax import lax
from jax.experimental import pallas as pl
from jax.experimental.pallas import tpu as pltpu
from jax.sharding import PartitionSpec as P

shift_mass = 0.05
jacobi_weight = 2.0 / 3.0
MESH = pl.DeviceIdType.MESH
ORB, FIRST, LEV_A, LEV_B, TWO_A, TWO_B, TWO_C = range(7)


def kernel(sizes, chunks, centre_in, half_width_in, pot_in, orbitals, out, *scratch):
    ext = scratch[0:7]
    second, zsend, zrecv, band_a, band_i, pot_b, d1_b, r1_b, r2_b = scratch[7:16]
    load_sem, store_sem, send_sem, recv_sem = scratch[16:20]
    centre, half_width, pot, small_sem = scratch[20:24]
    packed_out, packed_in = scratch[24:29], scratch[29:34]
    bands, nx, ny, nz = second.shape[2], second.shape[0], second.shape[1], second.shape[3]
    width = bands // chunks
    groups = width // 8
    two_sided = sizes["gz"] > 2
    dims = [(nx, ny, 1)] * 2 + [(nx // 2, ny // 2, 2)] * 2 + [(nx // 4, ny // 4, 4)] * 3
    lane = lax.broadcasted_iota(jnp.int32, (8, nz), 1)
    sub = lax.broadcasted_iota(jnp.int32, (8, nz), 0)

    near = {}
    for axis in ("gx", "gy", "gz"):
        me, n = lax.axis_index(axis), sizes[axis]
        near[axis] = ({axis: lax.rem(me + n - 1, n)}, {axis: lax.rem(me + 1, n)})
    peers = [near["gx"][0], near["gx"][1], near["gy"][0], near["gy"][1], near["gz"][1]]
    if two_sided:
        peers.append(near["gz"][0])

    smalls = [
        pltpu.make_async_copy(src, dst, small_sem.at[j])
        for j, (src, dst) in enumerate(
            [(centre_in, centre), (half_width_in, half_width), (pot_in, pot)]
        )
    ]

    def loads(k):
        rows = pl.ds(pl.multiple_of(k * width, 8), width)

        def line(x, _):
            for y in range(ny):
                pltpu.make_async_copy(
                    orbitals.at[rows, x, y], ext[ORB].at[x + 1, y + 1, rows], load_sem.at[k]
                ).start()
            return 0

        lax.fori_loop(0, nx, line, 0)

    lax.fori_loop(0, chunks, lambda k, c: (loads(k), c)[1], 0)
    for small in smalls:
        small.start()

    barrier = pltpu.get_barrier_semaphore()
    for peer in peers:
        pl.semaphore_signal(barrier, inc=1, device_id=peer, device_id_type=MESH)

    def copies(p, k):
        mx, my, _ = dims[p]
        e = ext[p]
        rows = pl.ds(pl.multiple_of(k * width, 8), width)
        ys, xs = pl.ds(1, my), pl.ds(1, mx)
        if p in (ORB, FIRST):
            moves = [
                (e.at[xs, 1, rows], e.at[xs, my + 1, rows], near["gy"][0]),
                (e.at[xs, my, rows], e.at[xs, 0, rows], near["gy"][1]),
                (e.at[1, ys, rows], e.at[mx + 1, ys, rows], near["gx"][0]),
                (e.at[mx, ys, rows], e.at[0, ys, rows], near["gx"][1]),
            ]
        else:
            share = width if p in (LEV_A, LEV_B) else width // 2
            part = pl.ds(pl.multiple_of(k * share, 8), share)
            sent, got = packed_out[p - LEV_A], packed_in[p - LEV_A]
            moves = [
                (sent.at[j, :, part], got.at[j, :, part], near[axis][side])
                for j, (axis, side) in enumerate(
                    [("gy", 0), ("gy", 1), ("gx", 0), ("gx", 1)]
                )
            ]
        moves.append((zsend.at[p, rows], zrecv.at[p, 0, rows], near["gz"][1]))
        if two_sided:
            moves.append((zsend.at[p, rows], zrecv.at[p, 1, rows], near["gz"][0]))
        return [
            pltpu.make_async_remote_copy(
                src_ref=src,
                dst_ref=dst,
                send_sem=send_sem.at[p, k, j],
                recv_sem=recv_sem.at[p, k, j],
                device_id=to,
                device_id_type=MESH,
            )
            for j, (src, dst, to) in enumerate(moves)
        ]

    def items(p, k):
        mx, my, w = dims[p]
        base = k * width
        if w == 2:
            for i in range(width // 8):
                at = pl.ds(pl.multiple_of(base + 8 * i, 8), 8)
                for pair in range(mx // 2):
                    yield pair, at, [(2 * pair, at), (2 * pair + 1, at)]
        else:
            for i in range(width // 16):
                rows = [pl.ds(pl.multiple_of(base + 16 * i + 8 * h, 8), 8) for h in (0, 1)]
                at = pl.ds(pl.multiple_of(k * (width // 2) + 8 * i, 8), 8)
                for pair in range(mx // 2):
                    yield pair, at, [(2 * pair + c, r) for r in rows for c in (0, 1)]

    def face_cell(p, j, cell, halo):
        mx, my, _ = dims[p]
        if j < 2:
            return (cell + 1, ((my + 1, 0) if halo else (1, my))[j])
        return (((mx + 1, 0) if halo else (1, mx))[j - 2], cell + 1)

    def send(p, k):
        if p not in (ORB, FIRST):
            w = dims[p][2]
            for pair, at, parts in items(p, k):
                for j in range(4):
                    acc = None
                    for spot, (cell, r) in enumerate(parts):
                        cx, cy = face_cell(p, j, cell, False)
                        v = ext[p][cx, cy, r]
                        acc = v if acc is None else jnp.where((lane & (w - 1)) == spot, v, acc)
                    packed_out[p - LEV_A][j, pair, at] = acc
        for copy in copies(p, k):
            copy.start()

    def receive(p, k):
        for copy in copies(p, k):
            copy.wait_recv()
        if p not in (ORB, FIRST):
            w = dims[p][2]
            for pair, at, parts in items(p, k):
                for j in range(4):
                    got = packed_in[p - LEV_A][j, pair, at]
                    for spot, (cell, r) in enumerate(parts):
                        cx, cy = face_cell(p, j, cell, True)
                        v = jnp.where((lane & (w - 1)) == spot, got, 0.0)
                        reach = 1
                        while reach < w:
                            v = v + roll(v, -reach if spot & reach else reach)
                            reach *= 2
                        ext[p][cx, cy, r] = v

    def roll(v, shift):
        return pltpu.roll(v, shift % nz, v.ndim - 1)

    def pack(p, get):
        mx, my, w = dims[p]
        acc = jnp.zeros((8, nz), jnp.float32)
        for x in range(mx):
            for y in range(my):
                at = 2 * w * (x * my + y)
                here = (lane >= at) & (lane < at + 2 * w)
                acc = jnp.where(here, roll(get(x, y), at + w), acc)
        return acc

    def pack_store(p, sl):
        zsend[p, sl] = pack(p, lambda x, y: ext[p][x + 1, y + 1, sl])

    def edges(p, sl):
        w = dims[p][2]
        got = zrecv[p, 0, sl]
        if two_sided:
            got = jnp.where((lane & (2 * w - 1)) < w, got, zrecv[p, 1, sl])
        return got

    def edge_at(p, got, x, y):
        _, my, w = dims[p]
        return roll(got, -(2 * w * (x * my + y)) - w)

    def along_z(v, h, w):
        low = roll(jnp.where(lane[None] >= nz - w, h, v), w)
        high = roll(jnp.where(lane[None] < w, h, v), -w)
        return low + high

    def around(p, sl, got, x):
        _, my, w = dims[p]
        e = ext[p]
        c = e[x + 1, pl.ds(1, my), sl]
        total = e[x, pl.ds(1, my), sl] + e[x + 2, pl.ds(1, my), sl]
        total = total + (e[x + 1, pl.ds(0, my), sl] + e[x + 1, pl.ds(2, my), sl])
        h = jnp.stack([edge_at(p, got, x, y) for y in range(my)])
        return c, total + along_z(c, h, w)

    def pair_sum(v, w):
        even = (lane & (2 * w - 1)) < w
        return v + jnp.where(even, roll(v, -w), roll(v, w))

    def each(body, p_in, p_out):
        def one(k, carry):
            if p_in is not None:
                receive(p_in, k)

            def inner(i, c):
                body(pl.ds(pl.multiple_of(k * width + i * 8, 8), 8))
                return c

            lax.fori_loop(0, groups, inner, 0)
            if p_out is not None:
                send(p_out, k)
            return carry

        lax.fori_loop(0, chunks, one, 0)

    pl.semaphore_wait(barrier, len(peers))

    def start(k, carry):
        rows = pl.ds(pl.multiple_of(k * width, 8), width)
        whole = ext[ORB].at[pl.ds(1, nx), pl.ds(1, ny), rows]
        pltpu.make_async_copy(whole, whole, load_sem.at[k]).wait()

        moves = copies(ORB, k)
        for copy in moves[:4]:
            copy.start()

        def inner(i, c):
            pack_store(ORB, pl.ds(pl.multiple_of(k * width + i * 8, 8), 8))
            return c

        lax.fori_loop(0, groups, inner, 0)
        for copy in moves[4:]:
            copy.start()
        return carry

    lax.fori_loop(0, chunks, start, 0)

    for small in smalls:
        small.wait()
    for g in range(bands // 8):
        m = jnp.zeros((8, nz), jnp.float32)
        s = jnp.ones((8, nz), jnp.float32)
        for j in range(8):
            m = jnp.where(sub == j, centre[g * 8 + j], m)
            s = jnp.where(sub == j, half_width[g * 8 + j], s)
        band_a[pl.ds(g * 8, 8)] = 3.0 - m
        band_i[pl.ds(g * 8, 8)] = 1.0 / s
    for x in range(nx):
        for y in range(ny):
            pot_b[x, y] = jnp.broadcast_to(pot[x, pl.ds(y, 1), :], (8, nz))
    for qx in range(nx // 4):
        for qy in range(ny // 4):
            quad = jnp.zeros((8, nz), jnp.float32)
            for hx in range(2):
                for hy in range(2):
                    x, y = 2 * qx + hx, 2 * qy + hy
                    v = pot_b[2 * x, 2 * y] + pot_b[2 * x + 1, 2 * y]
                    v = v + (pot_b[2 * x, 2 * y + 1] + pot_b[2 * x + 1, 2 * y + 1])
                    one = 0.125 * pair_sum(v, 1)
                    quad = quad + one
                    d1 = 0.75 + one + shift_mass
                    d1_b[x, y] = d1
                    r1_b[x, y] = jacobi_weight / d1
            r2_b[qx, qy] = jacobi_weight / (0.1875 + 0.125 * pair_sum(quad, 2) + shift_mass)

    def step_first(sl):
        got = edges(ORB, sl)
        a, i = band_a[sl], band_i[sl]
        for x in range(nx):
            c, total = around(ORB, sl, got, x)
            ext[FIRST][x + 1, pl.ds(1, ny), sl] = ((pot_b[x] + a) * c - 0.5 * total) * i
        pack_store(FIRST, sl)

    each(step_first, ORB, FIRST)

    def step_second(sl):
        got = edges(FIRST, sl)
        a, i = band_a[sl], 2.0 * band_i[sl]
        for x2 in range(nx // 2):
            pair = None
            for x in (2 * x2, 2 * x2 + 1):
                c, total = around(FIRST, sl, got, x)
                v = ((pot_b[x] + a) * c - 0.5 * total) * i - ext[ORB][x + 1, pl.ds(1, ny), sl]
                second[x, :, sl] = v
                pair = v if pair is None else pair + v
            for y2 in range(ny // 2):
                s = 0.5 * pair_sum(pair[2 * y2] + pair[2 * y2 + 1], 1)
                ext[LEV_A][x2 + 1, y2 + 1, sl] = r1_b[x2, y2] * s
        pack_store(LEV_A, sl)

    each(step_second, FIRST, LEV_A)

    def step_level(sl):
        got = edges(LEV_A, sl)
        for x in range(nx // 2):
            c, total = around(LEV_A, sl, got, x)
            ext[LEV_B][x + 1, pl.ds(1, ny // 2), sl] = (
                (2.0 - jacobi_weight) * c + 0.125 * r1_b[x] * total
            )
        pack_store(LEV_B, sl)

    each(step_level, LEV_A, LEV_B)

    def step_residue(sl):
        got = edges(LEV_B, sl)
        for x2 in range(nx // 4):
            pair = None
            for x in (2 * x2, 2 * x2 + 1):
                c, total = around(LEV_B, sl, got, x)
                d = d1_b[x]
                source = ext[LEV_A][x + 1, pl.ds(1, ny // 2), sl] * (d * (1.0 / jacobi_weight))
                v = source - d * c + 0.125 * total
                pair = v if pair is None else pair + v
            for y2 in range(ny // 4):
                s = 0.5 * pair_sum(pair[2 * y2] + pair[2 * y2 + 1], 2)
                ext[TWO_A][x2 + 1, y2 + 1, sl] = r2_b[x2, y2] * s
        pack_store(TWO_A, sl)

    each(step_residue, LEV_B, TWO_A)

    def step_two(sl):
        got = edges(TWO_A, sl)
        for x in range(nx // 4):
            c, total = around(TWO_A, sl, got, x)
            ext[TWO_B][x + 1, pl.ds(1, ny // 4), sl] = (
                (2.0 - jacobi_weight) * c + 0.03125 * r2_b[x] * total
            )
        pack_store(TWO_B, sl)

    each(step_two, TWO_A, TWO_B)

    def step_two_again(sl):
        got = edges(TWO_B, sl)
        for x in range(nx // 4):
            c, total = around(TWO_B, sl, got, x)
            scaled = ext[TWO_A][x + 1, pl.ds(1, ny // 4), sl]
            ext[TWO_C][x + 1, pl.ds(1, ny // 4), sl] = (
                (1.0 - jacobi_weight) * c + scaled + 0.03125 * r2_b[x] * total
            )
        pack_store(TWO_C, sl)

    each(step_two_again, TWO_B, TWO_C)

    def step_last(sl):
        hx, hy = nx // 2, ny // 2
        fine, coarse = ext[LEV_B], ext[TWO_C]

        def at(x, y):
            return fine[x + 1, y + 1, sl] + coarse[(x + 2) // 2, (y + 2) // 2, sl]

        got_one, got_two = edges(LEV_B, sl), edges(TWO_C, sl)
        for x in range(hx):
            for y in range(hy):
                c = at(x, y)
                total = (at(x - 1, y) + at(x + 1, y)) + (at(x, y - 1) + at(x, y + 1))
                h = edge_at(LEV_B, got_one, x, y) + edge_at(TWO_C, got_two, x // 2, y // 2)
                total = total + along_z(c[None], h[None], 2)[0]
                v = (1.0 - jacobi_weight) * c + ext[LEV_A][x + 1, y + 1, sl]
                v = v + 0.125 * r1_b[x, y] * total
                for i in range(2):
                    for j in range(2):
                        fx, fy = 2 * x + i, 2 * y + j
                        second[fx, fy, sl] = second[fx, fy, sl] + v

    def finish(k, carry):
        rows = pl.ds(pl.multiple_of(k * width, 8), width)
        receive(TWO_C, k)

        def inner(i, c):
            step_last(pl.ds(pl.multiple_of(k * width + i * 8, 8), 8))
            return c

        lax.fori_loop(0, groups, inner, 0)

        def line(x, c):
            for y in range(ny):
                pltpu.make_async_copy(
                    second.at[x, y, rows], out.at[rows, x, y], store_sem.at[k]
                ).start()
            return c

        lax.fori_loop(0, nx, line, 0)
        return carry

    lax.fori_loop(0, chunks, finish, 0)

    def drain(k, carry):
        rows = pl.ds(pl.multiple_of(k * width, 8), width)
        for p in range(7):
            for copy in copies(p, k):
                copy.wait_send()
        whole = second.at[:, :, rows]
        pltpu.make_async_copy(whole, whole, store_sem.at[k]).wait()
        return carry

    lax.fori_loop(0, chunks, drain, 0)


def local(sizes, chunks, orbitals, potential, centre, half_width):
    bands, nx, ny, nz = orbitals.shape

    def f32(*shape):
        return pltpu.VMEM(shape, jnp.float32)

    def padded(cut):
        return f32(nx // cut + 2, ny // cut + 2, bands, nz)

    scratch = [padded(1)] * 2 + [padded(2)] * 2 + [padded(4)] * 3
    scratch += [
        f32(nx, ny, bands, nz),
        f32(7, bands, nz),
        f32(7, 2, bands, nz),
        f32(bands, nz),
        f32(bands, nz),
        f32(nx, ny, 8, nz),
        f32(nx // 2, ny // 2, 8, nz),
        f32(nx // 2, ny // 2, 8, nz),
        f32(nx // 4, ny // 4, 8, nz),
        pltpu.SemaphoreType.DMA((chunks,)),
        pltpu.SemaphoreType.DMA((chunks,)),
        pltpu.SemaphoreType.DMA((7, chunks, 6)),
        pltpu.SemaphoreType.DMA((7, chunks, 6)),
        pltpu.SMEM((bands,), jnp.float32),
        pltpu.SMEM((bands,), jnp.float32),
        f32(nx, ny, nz),
        pltpu.SemaphoreType.DMA((3,)),
    ]
    for _ in range(2):
        scratch += [f32(4, max(nx, ny) // 4, bands, nz)] * 2
        scratch += [f32(4, max(nx, ny) // 8, bands // 2, nz)] * 3
    return pl.pallas_call(
        functools.partial(kernel, sizes, chunks),
        out_shape=jax.ShapeDtypeStruct(orbitals.shape, jnp.float32),
        in_specs=[pl.BlockSpec(memory_space=pltpu.HBM)] * 4,
        out_specs=pl.BlockSpec(memory_space=pl.ANY),
        scratch_shapes=scratch,
        compiler_params=pltpu.CompilerParams(
            collective_id=0, has_side_effects=True, vmem_limit_bytes=48 * 1024 * 1024
        ),
    )(*(pltpu.with_memory_space_constraint(v, pltpu.HBM) for v in (centre, half_width, potential, orbitals)))


def solution(mesh):
    in_specs = (P(None, "gx", "gy", "gz"), P("gx", "gy", "gz"), P(), P())
    out_specs = P(None, "gx", "gy", "gz")
    body = functools.partial(local, dict(mesh.shape), 4)
    return jax.shard_map(body, mesh=mesh, in_specs=in_specs, out_specs=out_specs, check_vma=False)
```
